256 devices in a mesh: south: 32 (over z, x), east: 8 (over y, core).
Axes of the slice: x: 4, y: 4, z: 8, core: 2. Of those that a mesh axis runs over, the one named last changes fastest.
Arguments:
- tracer: float32 [1024, 256, 128], P('south', 'east'), may hold values from 0.2 to 1.8
- flow_j: float32 [1024, 256, 128], P('south', 'east'), may hold values from -0.3 to 0.3
- flow_i: float32 [1024, 256, 128], P('south', 'east'), may hold values from -0.3 to 0.3
Outputs:
- running_total: float32 [1024, 256, 128], P('south', 'east')
- tracer_end: float32 [1024, 256, 128], P('south', 'east')
The draws below stay inside these ranges and needn't reach their ends.
All inputs are finite; a program needn't handle non-finite values.
Results may differ from the reference program's by a relative error of at most 0.00002.
Values sent between devices are 32-bit elements; how exact they have to be, the bound alone decides.
No kernel may reach another device: no remote copies, remote signals or barrier semaphores. Data moves between devices by JAX's collectives and lax.ppermute only.
A program may use at most 64 MiB of HBM per device.

```python
import jax
import jax.numpy as jnp
from jax import lax

GRID_J = 1024
GRID_I = 256
MEMBERS = 128
STEPS = 4


def level_of(key, shape, pieces, least, top_value):
    gain, own = 1.0, jax.random.fold_in(key, 6)
    for dim, blocks in pieces:
        heights = jnp.exp(jax.random.uniform(jax.random.fold_in(own, dim), (blocks,), jnp.float32, least / len(pieces), top_value / len(pieces)))
        gain = gain * jnp.repeat(heights, shape[dim] // blocks).reshape([-1 if axis == dim else 1 for axis in range(len(shape))])
    return gain


def setup_inputs(seed: int = 0) -> dict:
    keys = jax.random.split(jax.random.key(seed), 4)
    tracer = jnp.clip(0.2 + 1.5999999 * jax.random.uniform(keys[0], (GRID_J, GRID_I, MEMBERS), jnp.float32) ** level_of(keys[0], (GRID_J, GRID_I, MEMBERS), ((0, 32), (1, 8)), -0.2, 0.2), 0.2, 1.8)
    flow_j = jnp.clip(jax.random.uniform(keys[1], (GRID_J, GRID_I, MEMBERS), jnp.float32, -0.3, 0.3) * level_of(keys[1], (GRID_J, GRID_I, MEMBERS), ((0, 32), (1, 8)), -0.4, 0.0), -0.3, 0.3)
    flow_i = jnp.clip(jax.random.uniform(keys[2], (GRID_J, GRID_I, MEMBERS), jnp.float32, -0.3, 0.3) * level_of(keys[2], (GRID_J, GRID_I, MEMBERS), ((0, 32), (1, 8)), -0.4, 0.0), -0.3, 0.3)
    return {"tracer": tracer, "flow_j": flow_j, "flow_i": flow_i}


def inner_cells(values, dims):
    for dim in dims:
        values = lax.slice_in_dim(values, 1, values.shape[dim] - 1, axis=dim)
    return values


def side_cells(values, dim, start, dims):
    others = [other for other in dims if other != dim]
    values = inner_cells(values, others)
    return lax.slice_in_dim(values, start, start + values.shape[dim] - 2, axis=dim)


def advance(padded, flow_j, flow_i):
    middle = inner_cells(padded, (0, 1))
    lower = [side_cells(padded, dim, 0, (0, 1)) for dim in (0, 1)]
    upper = [side_cells(padded, dim, 2, (0, 1)) for dim in (0, 1)]
    slopes = [above - below for above, below in zip(upper, lower)]
    smooth_rate = 0.05
    spread = lower[0] + upper[0] + lower[1] + upper[1] - 4.0 * middle
    return middle - flow_j * slopes[0] - flow_i * slopes[1] + smooth_rate * spread


def reference(tracer, flow_j, flow_i):
    for step in range(STEPS):
        tracer = advance(jnp.pad(tracer, ((1, 1), (1, 1), (0, 0)), mode="constant"), flow_j, flow_i)
    running_total = jnp.cumsum(tracer, axis=0) / GRID_J
    return running_total, tracer
```

```python
import jax
import jax.numpy as jnp
from jax import lax
from jax.experimental import pallas as pl
from jax.experimental.pallas import tpu as pltpu
from jax.sharding import PartitionSpec as P

STEPS = 4
RATE = 0.05
ROW = 4


def exchange(array, axis, partner):
    size = lax.axis_size(axis)
    pairs = [(i, partner(i)) for i in range(size)]
    return lax.ppermute(array, axis, [(i, p) for i, p in pairs if 0 <= p < size])


def stencil_kernel(
    place, tracer, flow_j, flow_i, recv0, recv1, sides, corner0, corner1, edge,
    end, here, total, x, fj, fi,
):
    rows, cols = tracer.shape[0], tracer.shape[1]
    even, has_low, has_high = place[0], place[1], place[2]
    w = STEPS

    def own(j, carry):
        x[w + j, 0:cols] = tracer[j]
        x[w + j, cols:] = sides[0, j]
        fj[w + j, 0:cols] = flow_j[j]
        fj[w + j, cols:] = sides[1, j]
        fi[w + j, 0:cols] = flow_i[j]
        fi[w + j, cols:] = sides[2, j]
        return carry

    lax.fori_loop(0, rows, own, 0, unroll=4)

    def halo(recv, corner, low):
        base = 0 if low else w + rows
        inner = 1 if low else 0
        for d in range(w):
            x[base + d, 0:cols] = recv[d]
            x[base + d, cols:] = corner[0, d]
        for d in range(w - 1):
            fj[base + inner + d, 0:cols] = recv[w + d]
            fj[base + inner + d, cols:] = corner[1, inner + d]
            fi[base + inner + d, 0:cols] = recv[2 * w - 1 + d]
            fi[base + inner + d, cols:] = corner[2, inner + d]

    @pl.when(even == 1)
    def _():
        halo(recv0, corner0, False)
        halo(recv1, corner1, True)

    @pl.when(even == 0)
    def _():
        halo(recv1, corner1, False)
        halo(recv0, corner0, True)

    mask = edge[...]
    size = cols + 2 * w
    low_gain = has_low.astype(jnp.float32)
    high_gain = has_high.astype(jnp.float32)

    def advance(below, middle, above, r):
        right = pltpu.roll(middle, size - 1, 0)
        left = pltpu.roll(middle, 1, 0)
        spread = below + above + left + right - 4.0 * middle
        return middle - fj[r] * (above - below) - fi[r] * (right - left) + RATE * spread

    for step in range(STEPS - 1):
        first, last = step + 1, rows + 2 * w - 2 - step

        def body(r, carry, gain=None):
            below, middle = carry
            above = x[r + 1]
            new = advance(below, middle, above, r) * mask
            x[r] = new if gain is None else new * gain
            return middle, above

        carry = (x[first - 1], x[first])
        for r in range(first, w):
            carry = body(r, carry, low_gain)
        carry = lax.fori_loop(w, w + rows, body, carry, unroll=4)
        for r in range(w + rows, last + 1):
            carry = body(r, carry, high_gain)

    def final(j, carry):
        below, middle, so_far = carry
        above = x[w + j + 1]
        new = advance(below, middle, above, w + j)[0:cols]
        so_far = so_far + new
        end[j] = new
        here[j] = so_far
        return middle, above, so_far

    carry = (x[w - 1], x[w], jnp.zeros((cols, tracer.shape[2]), jnp.float32))
    total[...] = lax.fori_loop(0, rows, final, carry, unroll=4)[2]


def per_device(tracer, flow_j, flow_i):
    rows, cols, members = tracer.shape
    south, east = lax.axis_index("south"), lax.axis_index("east")
    n_south, n_east = lax.axis_size("south"), lax.axis_size("east")
    even_s, even_e = south % 2 == 0, east % 2 == 0
    w = STEPS
    arrays = (tracer, flow_j, flow_i)

    def even_partner(i):
        return i ^ 1

    def odd_partner(size, wrap):
        def partner(i):
            p = i + 1 if i % 2 else i - 1
            return p % size if wrap else p
        return partner

    lefts = jnp.stack([a[:, :w] for a in arrays])
    rights = jnp.stack([a[:, cols - w:] for a in arrays])
    e0 = exchange(jnp.where(even_e, rights, lefts), "east", even_partner)
    e1 = exchange(jnp.where(even_e, lefts, rights), "east", odd_partner(n_east, True))

    def edge_rows(high):
        def cut(a, n):
            start = jnp.where(high, rows - n, 0)
            return lax.dynamic_slice(a, (start, 0, 0), (n, cols, members))
        return jnp.concatenate([cut(tracer, w), cut(flow_j, w - 1), cut(flow_i, w - 1)])

    s1 = exchange(edge_rows(~even_s), "south", odd_partner(n_south, False))
    s0 = exchange(edge_rows(even_s), "south", even_partner)

    right = jnp.where(even_e, e0, e1)
    left = jnp.where(even_e, e1, e0)
    in_left, in_right = east > 0, east < n_east - 1
    sides = jnp.concatenate(
        [jnp.where(in_right, right, 0.0), jnp.where(in_left, left, 0.0)], axis=2
    )

    def edge_sides(high):
        start = jnp.where(high, rows - w, 0)
        return lax.dynamic_slice(sides, (0, start, 0, 0), (3, w, 2 * w, members))

    c1 = exchange(edge_sides(~even_s), "south", odd_partner(n_south, False))
    c0 = exchange(edge_sides(even_s), "south", even_partner)

    column = lax.broadcasted_iota(jnp.int32, (cols + 2 * w, members), 0)
    edge = jnp.where(
        column < cols, 1.0, jnp.where(column < cols + w, in_right, in_left).astype(jnp.float32)
    )
    place = jnp.stack([even_s, south > 0, south < n_south - 1]).astype(jnp.int32)
    size = (rows + 2 * w, cols + 2 * w, members)
    vmem = pl.BlockSpec(memory_space=pltpu.VMEM)
    end, here, total = pl.pallas_call(
        stencil_kernel,
        out_shape=(
            jax.ShapeDtypeStruct(tracer.shape, jnp.float32),
            jax.ShapeDtypeStruct(tracer.shape, jnp.float32),
            jax.ShapeDtypeStruct((cols, members), jnp.float32),
        ),
        in_specs=[pl.BlockSpec(memory_space=pltpu.SMEM)] + [vmem] * 9,
        out_specs=(vmem, vmem, vmem),
        scratch_shapes=[pltpu.VMEM(size, jnp.float32)] * 3,
        compiler_params=pltpu.CompilerParams(vmem_limit_bytes=16 * 1024 * 1024),
        name="stencil",
    )(place, tracer, flow_j, flow_i, s0, s1, sides, c0, c1, edge)

    column_of, row_of = south % ROW, south // ROW
    rounds = (
        (lambda i: i ^ 1, column_of & 1),
        (lambda i: i ^ 3, column_of >> 1),
        (lambda i: i ^ 4, row_of & 1),
        (lambda i: i ^ 8, (row_of >> 1) & 1),
        (lambda i: i ^ 28, row_of >> 2),
    )
    before = jnp.zeros_like(total)
    for partner, upper in rounds:
        other = exchange(total, "south", partner)
        before = before + jnp.where(upper == 1, other, 0.0)
        total = total + other
    running_total = (here + before) * (1.0 / (rows * n_south))
    return running_total, end


def solution(mesh):
    spec = P("south", "east", None)
    return jax.shard_map(
        per_device, mesh=mesh, in_specs=(spec,) * 3, out_specs=(spec,) * 2, check_vma=False
    )
```

```python
import jax
import jax.numpy as jnp
from jax import lax
from jax.experimental import pallas as pl
from jax.experimental.pallas import tpu as pltpu
from jax.sharding import PartitionSpec as P

STEPS = 4
RATE = 0.05
ROW = 4
TILE = 8
W = STEPS

VMEM = pl.BlockSpec(memory_space=pltpu.VMEM)
ANY = pl.BlockSpec(memory_space=pl.ANY)
HBM = pl.BlockSpec(memory_space=pltpu.HBM)


def exchange(array, axis, partner):
    size = lax.axis_size(axis)
    pairs = [(i, partner(i)) for i in range(size)]
    return lax.ppermute(array, axis, [(i, p) for i, p in pairs if 0 <= p < size])


def even_partner(i):
    return i ^ 1


def odd_partner(size, wrap):
    def partner(i):
        p = i + 1 if i % 2 else i - 1
        return p % size if wrap else p
    return partner


def call(kernel, name, outs, operands, in_specs, scratch=(), cost=0, aliases=None, result=()):
    return pl.pallas_call(
        kernel,
        out_shape=tuple(
            (jax.ShapeDtypeStruct if i in result else pltpu.VMEM)(s, jnp.float32)
            for i, s in enumerate(outs)
        ),
        in_specs=in_specs,
        out_specs=(VMEM,) * len(outs),
        scratch_shapes=scratch,
        compiler_params=pltpu.CompilerParams(vmem_limit_bytes=16 << 20),
        cost_estimate=pl.CostEstimate(flops=cost, bytes_accessed=cost, transcendentals=0),
        input_output_aliases=aliases or {},
        name=name,
    )(*operands)


def low_half(shape):
    return lax.broadcasted_iota(jnp.int32, shape, len(shape) - 2) < W


def place_of():
    south, east = lax.axis_index("south"), lax.axis_index("east")
    n_south, n_east = lax.axis_size("south"), lax.axis_size("east")
    conditions = (
        south % 2 == 0, east % 2 == 0, east < n_east - 1, east > 0, south > 0, south < n_south - 1
    )
    return tuple(c.astype(jnp.int32) for c in conditions)


def pack_kernel(tracer, flow_j, flow_i, s0, s1, e0, e1, left, right, sems):
    rows, cols = tracer.shape[0], tracer.shape[1]
    even_s, even_e = place_of()[:2]
    arrays = (tracer, flow_j, flow_i)
    copies = []

    def copy(src, dst):
        c = pltpu.make_async_copy(src, dst, sems.at[len(copies)])
        c.start()
        copies.append(c)

    for k, a in enumerate(arrays):
        copy(a.at[:, pl.ds(0, TILE)], left.at[k])
        copy(a.at[:, pl.ds(cols - TILE, TILE)], right.at[k])
    at = 0
    for a, n in zip(arrays, (W, W - 1, W - 1)):
        high = rows - n
        copy(a.at[pl.ds(even_s * high, n)], s0.at[pl.ds(at, n)])
        copy(a.at[pl.ds((1 - even_s) * high, n)], s1.at[pl.ds(at, n)])
        at += n
    for c in copies[:6]:
        c.wait()
    half = rows // 2
    low = low_half((TILE, tracer.shape[2]))

    def fold(j, carry):
        for k in range(3):
            lo = jnp.where(low, left[k, j], pltpu.roll(left[k, j + half], W, 0))
            hi = jnp.where(low, pltpu.roll(right[k, j], W, 0), right[k, j + half])
            e0[k, j] = jnp.where(even_e == 1, hi, lo)
            e1[k, j] = jnp.where(even_e == 1, lo, hi)
        return carry

    lax.fori_loop(0, half, fold, 0, unroll=4)
    for c in copies[6:]:
        c.wait()


def unfolded(e0, e1, k, j):
    _, even_e, in_right, in_left, *_ = place_of()
    low = low_half(e0.shape[2:])
    gain = jnp.where(low, in_right, in_left).astype(jnp.float32)
    a, b = e0[k, j], e1[k, j]
    right = jnp.where(even_e == 1, a, b)
    left = jnp.where(even_e == 1, b, a)
    return (
        jnp.where(low, right, pltpu.roll(left, W, 0)) * gain,
        jnp.where(low, pltpu.roll(right, W, 0), left) * gain,
    )


def corner_kernel(e0, e1, c0, c1):
    half = e0.shape[1]
    even_s = place_of()[0]
    for k in range(3):
        for d in range(W):
            first = unfolded(e0, e1, k, d)[0]
            last = unfolded(e0, e1, k, half - W + d)[1]
            c0[k, d] = jnp.where(even_s == 1, last, first)
            c1[k, d] = jnp.where(even_s == 1, first, last)


def fill_kernel(tracer, flow_j, flow_i, e0, e1, x, fj, fi, sems):
    rows, cols = tracer.shape[0], tracer.shape[1]
    half = rows // 2
    copies = []
    for k, (src, dst) in enumerate(((tracer, x), (flow_j, fj), (flow_i, fi))):
        inner = dst.at[pl.ds(W, rows), pl.ds(0, cols)]
        copies.append(pltpu.make_async_copy(src, inner, sems.at[k]))
    for c in copies:
        c.start()

    def body(j, carry):
        for k, dst in enumerate((x, fj, fi)):
            near, far = unfolded(e0, e1, k, j)
            dst[W + j, cols:] = near
            dst[W + half + j, cols:] = far
        return carry

    lax.fori_loop(0, half, body, 0, unroll=4)
    for c in copies:
        c.wait()


def stencil_kernel(
    recv0, recv1, corner0, corner1, x_in, fj_in, fi_in, x, fj, fi, end, total
):
    del x_in, fj_in, fi_in
    rows, cols = end.shape[0], end.shape[1]
    even_s, _, in_right, in_left, has_low, has_high = place_of()

    low_gain = has_low.astype(jnp.float32)
    high_gain = has_high.astype(jnp.float32)

    def halo(recv, corner, low):
        base = 0 if low else W + rows
        gain = low_gain if low else high_gain
        inner = 1 if low else 0
        for d in range(W):
            x[base + d, 0:cols] = recv[d] * gain
            x[base + d, cols:] = corner[0, d] * gain
        for d in range(W - 1):
            fj[base + inner + d, 0:cols] = recv[W + d]
            fj[base + inner + d, cols:] = corner[1, inner + d]
            fi[base + inner + d, 0:cols] = recv[2 * W - 1 + d]
            fi[base + inner + d, cols:] = corner[2, inner + d]

    @pl.when(even_s == 1)
    def _():
        halo(recv0, corner0, False)
        halo(recv1, corner1, True)

    @pl.when(even_s == 0)
    def _():
        halo(recv1, corner1, False)
        halo(recv0, corner0, True)

    size = cols + 2 * W
    column = lax.broadcasted_iota(jnp.int32, (size, x.shape[2]), 0)
    side = jnp.where(column < cols + W, in_right, in_left).astype(jnp.float32)
    mask = jnp.where(column < cols, 1.0, side)

    def advance(below, middle, above, r):
        right = pltpu.roll(middle, size - 1, 0)
        left = pltpu.roll(middle, 1, 0)
        spread = below + above + left + right - 4.0 * middle
        return middle - fj[r] * (above - below) - fi[r] * (right - left) + RATE * spread

    for step in range(STEPS - 1):
        first, last = step + 1, rows + 2 * W - 2 - step

        def body(r, carry, gain=None):
            below, middle = carry
            above = x[r + 1]
            new = advance(below, middle, above, r)
            new = jnp.concatenate([new[:cols], new[cols:] * mask[cols:]], axis=0)
            x[r] = new if gain is None else new * gain
            return middle, above

        carry = (x[first - 1], x[first])
        for r in range(first, W):
            carry = body(r, carry, low_gain)
        carry = lax.fori_loop(W, W + rows, body, carry, unroll=4)
        for r in range(W + rows, last + 1):
            carry = body(r, carry, high_gain)

    def final(j, carry):
        below, middle, so_far = carry
        above = x[W + j + 1]
        new = advance(below, middle, above, W + j)[0:cols]
        end[j] = new
        return middle, above, so_far + new

    carry = (x[W - 1], x[W], jnp.zeros((cols, x.shape[2]), jnp.float32))
    total[...] = lax.fori_loop(0, rows, final, carry, unroll=4)[2]


def sums_kernel(scale, end, here, copied):
    def body(j, so_far):
        row = end[j]
        copied[j] = row
        so_far = so_far + row
        here[j] = so_far * scale
        return so_far

    lax.fori_loop(0, end.shape[0], body, jnp.zeros(end.shape[1:], jnp.float32), unroll=4)


def per_device(tracer, flow_j, flow_i):
    rows, cols, members = tracer.shape
    south, east = lax.axis_index("south"), lax.axis_index("east")
    n_south, n_east = lax.axis_size("south"), lax.axis_size("east")
    fields = tuple(pltpu.with_memory_space_constraint(a, pltpu.HBM) for a in (tracer, flow_j, flow_i))
    edge = (3 * W - 2, cols, members)
    fold = (3, rows // 2, TILE, members)
    s0, s1, e0, e1 = call(
        pack_kernel, "pack", (edge, edge, fold, fold), fields, [HBM] * 3,
        [pltpu.VMEM((3, rows, TILE, members), jnp.float32)] * 2 + [pltpu.SemaphoreType.DMA((12,))],
    )
    e1 = exchange(e1, "east", odd_partner(n_east, True))
    e0 = exchange(e0, "east", even_partner)
    s1 = exchange(s1, "south", odd_partner(n_south, True))
    s0 = exchange(s0, "south", even_partner)

    corner = (3, W, TILE, members)
    c0, c1 = call(
        corner_kernel, "corners", (corner, corner), (e0, e1), [VMEM] * 2
    )
    c1 = exchange(c1, "south", odd_partner(n_south, True))
    c0 = exchange(c0, "south", even_partner)

    size = (rows + 2 * W, cols + 2 * W, members)
    wide = call(
        fill_kernel, "fill", (size,) * 3, (*fields, e0, e1), [HBM] * 3 + [VMEM] * 2,
        [pltpu.SemaphoreType.DMA((3,))], cost=1 << 22,
    )
    *_, end, total = call(
        stencil_kernel, "stencil", (size,) * 3 + (tracer.shape, (cols, members)),
        (s0, s1, c0, c1, *wide), [VMEM] * 7,
        aliases={4: 0, 5: 1, 6: 2},
    )
    scale = 1.0 / (rows * n_south)

    here, end = call(
        lambda *refs: sums_kernel(scale, *refs), "sums", (tracer.shape,) * 2, (end,), [VMEM],
        cost=1 << 21, result=(1,),
    )

    before = jnp.zeros_like(total)
    for flips in ((1, 3, 2), (4, 12, 8), (28,)):
        parts = [exchange(total, "south", lambda i, k=k: i ^ k) for k in flips]
        for k, part in zip(flips, parts):
            before = before + jnp.where((south ^ k) < south, part, 0.0)
        total = total + sum(parts)
    return here + before * scale, end


def solution(mesh):
    spec = P("south", "east", None)
    return jax.shard_map(
        per_device, mesh=mesh, in_specs=(spec,) * 3, out_specs=(spec,) * 2, check_vma=False
    )
```

```python
import jax
import jax.numpy as jnp
from jax import lax
from jax.experimental import pallas as pl
from jax.experimental.pallas import tpu as pltpu
from jax.sharding import PartitionSpec as P

STEPS = 4
RATE = 0.05
ROW = 4
TILE = 8
W = STEPS

VMEM = pl.BlockSpec(memory_space=pltpu.VMEM)
ANY = pl.BlockSpec(memory_space=pl.ANY)
HBM = pl.BlockSpec(memory_space=pltpu.HBM)


def exchange(array, partner):
    n_south, n_east = lax.axis_size("south"), lax.axis_size("east")
    pairs = []
    for i in range(n_south):
        for j in range(n_east):
            p, q = partner(i, j)
            pairs.append((i * n_east + j, p * n_east + q))
    return lax.ppermute(array, ("south", "east"), pairs)


def odd(i):
    return i + 1 if i % 2 else i - 1


def south_even(i, j):
    return i ^ 1, j


def south_odd(i, j):
    p = odd(i)
    inside = 0 <= p < lax.axis_size("south")
    return (p, j) if inside else (i, j ^ 1)


def east_even(i, j):
    return i, j ^ 1


def east_odd(i, j):
    q = odd(j)
    return i, q % lax.axis_size("east")


def call(kernel, name, outs, operands, in_specs, scratch=(), cost=0, aliases=None, result=()):
    return pl.pallas_call(
        kernel,
        out_shape=tuple(
            (jax.ShapeDtypeStruct if i in result else pltpu.VMEM)(s, jnp.float32)
            for i, s in enumerate(outs)
        ),
        in_specs=in_specs,
        out_specs=(VMEM,) * len(outs),
        scratch_shapes=scratch,
        compiler_params=pltpu.CompilerParams(vmem_limit_bytes=16 << 20),
        cost_estimate=pl.CostEstimate(flops=cost, bytes_accessed=cost, transcendentals=0),
        input_output_aliases=aliases or {},
        name=name,
    )(*operands)


def low_half(shape):
    return lax.broadcasted_iota(jnp.int32, shape, len(shape) - 2) < W


def place_of():
    south, east = lax.axis_index("south"), lax.axis_index("east")
    n_south, n_east = lax.axis_size("south"), lax.axis_size("east")
    conditions = (
        south % 2 == 0, east % 2 == 0, east < n_east - 1, east > 0, south > 0, south < n_south - 1
    )
    return tuple(c.astype(jnp.int32) for c in conditions)


def start_all(copies):
    for c in copies:
        c.start()
    return copies


def wait_all(copies):
    for c in copies:
        c.wait()


def pack_kernel(tracer, flow_j, flow_i, s0, s1, e0, e1, left, right, sems):
    rows, cols = tracer.shape[0], tracer.shape[1]
    even_s, even_e = place_of()[:2]
    arrays = (tracer, flow_j, flow_i)
    copies = []

    def copy(src, dst):
        c = pltpu.make_async_copy(src, dst, sems.at[len(copies)])
        c.start()
        copies.append(c)

    for k, a in enumerate(arrays):
        copy(a.at[:, pl.ds(0, TILE)], left.at[k])
        copy(a.at[:, pl.ds(cols - TILE, TILE)], right.at[k])
    at = 0
    for a, n in zip(arrays, (W, W - 1, W - 1)):
        high = rows - n
        copy(a.at[pl.ds(even_s * high, n)], s0.at[pl.ds(at, n)])
        copy(a.at[pl.ds((1 - even_s) * high, n)], s1.at[pl.ds(at, n)])
        at += n
    for c in copies[:6]:
        c.wait()
    half = rows // 2
    low = low_half((TILE, tracer.shape[2]))

    def fold(j, carry):
        for k in range(3):
            lo = jnp.where(low, left[k, j], pltpu.roll(left[k, j + half], W, 0))
            hi = jnp.where(low, pltpu.roll(right[k, j], W, 0), right[k, j + half])
            e0[k, j] = jnp.where(even_e == 1, hi, lo)
            e1[k, j] = jnp.where(even_e == 1, lo, hi)
        return carry

    lax.fori_loop(0, half, fold, 0, unroll=4)
    for c in copies[6:]:
        c.wait()


def unfolded(e0, e1, k, j):
    _, even_e, in_right, in_left, *_ = place_of()
    low = low_half(e0.shape[2:])
    gain = jnp.where(low, in_right, in_left).astype(jnp.float32)
    a, b = e0[k, j], e1[k, j]
    right = jnp.where(even_e == 1, a, b)
    left = jnp.where(even_e == 1, b, a)
    return (
        jnp.where(low, right, pltpu.roll(left, W, 0)) * gain,
        jnp.where(low, pltpu.roll(right, W, 0), left) * gain,
    )


def corner_kernel(e0, e1, c0, c1):
    half = e0.shape[1]
    even_s = place_of()[0]
    for k in range(3):
        for d in range(W):
            first = unfolded(e0, e1, k, d)[0]
            last = unfolded(e0, e1, k, half - W + d)[1]
            c0[k, d] = jnp.where(even_s == 1, last, first)
            c1[k, d] = jnp.where(even_s == 1, first, last)


def side_mask(shape):
    in_right, in_left = place_of()[2:4]
    return jnp.where(low_half(shape), in_right, in_left).astype(jnp.float32)


def advance(below, middle, above, flow_j, flow_i, mask):
    size, cols = middle.shape[0], middle.shape[0] - TILE
    right = pltpu.roll(middle, size - 1, 0)
    left = pltpu.roll(middle, 1, 0)
    spread = below + above + left + right - 4.0 * middle
    new = middle - flow_j * (above - below) - flow_i * (right - left) + RATE * spread
    return jnp.concatenate([new[:cols], new[cols:] * mask], axis=0)


def inner_kernel(tracer, flow_j, flow_i, e0, e1, fj, fi, kept, end, total, x, sems):
    rows, cols = tracer.shape[0], tracer.shape[1]
    half = rows // 2
    wide = ((tracer, x), (flow_j, fj), (flow_i, fi))
    copies = start_all([
        pltpu.make_async_copy(src, dst.at[:, pl.ds(0, cols)], sems.at[k])
        for k, (src, dst) in enumerate(wide)
    ])

    def sides(j, carry):
        for k, (_, dst) in enumerate(wide):
            near, far = unfolded(e0, e1, k, j)
            dst[j, cols:] = near
            dst[half + j, cols:] = far
        return carry

    lax.fori_loop(0, half, sides, 0, unroll=4)
    wait_all(copies)
    mask = side_mask((TILE, x.shape[2]))

    for step in range(1, STEPS + 1):
        first, last = step, rows - 1 - step
        for n in range(2):
            kept[step - 1, 0, n] = x[first - 1 + n]
            kept[step - 1, 1, n] = x[last + 1 - n]

        def body(r, carry):
            below, middle = carry[:2]
            above = x[r + 1]
            new = advance(below, middle, above, fj[r], fi[r], mask)
            if step < STEPS:
                x[r] = new
                return middle, above
            end[r] = new[:cols]
            return middle, above, carry[2] + new[:cols]

        carry = (x[first - 1], x[first])
        if step == STEPS:
            carry += (jnp.zeros((cols, x.shape[2]), jnp.float32),)
        carry = lax.fori_loop(first, last + 1, body, carry, unroll=4)
    total[...] = carry[2]


def outer_kernel(
    recv0, recv1, corner0, corner1, fj, fi, kept, inner_end, inner_total, end, total
):
    del inner_end
    rows, cols = end.shape[0], end.shape[1]
    even_s, _, _, _, has_low, has_high = place_of()
    mask = side_mask((TILE, end.shape[2]))
    so_far = inner_total[...]

    for low in (True, False):
        ours = even_s == (0 if low else 1)
        gain = (has_low if low else has_high).astype(jnp.float32)

        def halo(at, k, d):
            return jnp.concatenate([
                jnp.where(ours, recv0[at], recv1[at]), jnp.where(ours, corner0[k, d], corner1[k, d])
            ], axis=0)

        order = [W - 1 - d for d in range(W)] if low else list(range(W))
        field = [halo(d, 0, d) * gain for d in order]
        flows = []
        for k, base in ((1, W), (2, 2 * W - 1)):
            flows.append([halo(base + (d - 1 if low else d), k, d) for d in order[:W - 1]])

        def flow(k, own, at):
            row = at if low else rows - 1 - at
            return flows[k][-1 - at] if at < 0 else own[row]

        values = field[::-1]
        for step in range(1, STEPS + 1):
            side = 0 if low else 1
            inward = values + [kept[step - 1, side, 0], kept[step - 1, side, 1]]
            values = []
            for n in range(1, W + 1):
                at = n - 1 + step - W
                outside, middle, inside = inward[n - 1:n + 2]
                below, above = (outside, inside) if low else (inside, outside)
                new = advance(
                    below, middle, above, flow(0, fj, at), flow(1, fi, at), mask
                )
                values.append(new * gain if at < 0 else new)
        for at, value in enumerate(values):
            end[at if low else rows - 1 - at] = value[:cols]
            so_far = so_far + value[:cols]
    total[...] = so_far


def sums_kernel(scale, end, here, copied):
    def body(j, so_far):
        row = end[j]
        copied[j] = row
        so_far = so_far + row
        here[j] = so_far * scale
        return so_far

    lax.fori_loop(0, end.shape[0], body, jnp.zeros(end.shape[1:], jnp.float32), unroll=4)


def per_device(tracer, flow_j, flow_i):
    rows, cols, members = tracer.shape
    south, east = lax.axis_index("south"), lax.axis_index("east")
    n_south, n_east = lax.axis_size("south"), lax.axis_size("east")
    fields = tuple(pltpu.with_memory_space_constraint(a, pltpu.HBM) for a in (tracer, flow_j, flow_i))
    edge = (3 * W - 2, cols, members)
    fold = (3, rows // 2, TILE, members)
    s0, s1, e0, e1 = call(
        pack_kernel, "pack", (edge, edge, fold, fold), fields, [HBM] * 3,
        [pltpu.VMEM((3, rows, TILE, members), jnp.float32)] * 2 + [pltpu.SemaphoreType.DMA((12,))],
    )
    e1 = exchange(e1, east_odd)
    e0 = exchange(e0, east_even)
    s1 = exchange(s1, south_odd)
    s0 = exchange(s0, south_even)

    corner = (3, W, TILE, members)
    c0, c1 = call(
        corner_kernel, "corners", (corner, corner), (e0, e1), [VMEM] * 2
    )
    c1 = exchange(c1, south_odd)
    c0 = exchange(c0, south_even)

    wide = (rows, cols + TILE, members)
    ends = (STEPS, 2, 2, cols + TILE, members)
    inner = call(
        inner_kernel, "inner", (wide, wide, ends, tracer.shape, (cols, members)),
        (*fields, e0, e1), [HBM] * 3 + [VMEM] * 2,
        [pltpu.VMEM(wide, jnp.float32), pltpu.SemaphoreType.DMA((3,))], cost=1 << 23,
    )
    end, total = call(
        outer_kernel, "outer", (tracer.shape, (cols, members)), (s0, s1, c0, c1, *inner),
        [VMEM] * 9, aliases={7: 0},
    )
    scale = 1.0 / (rows * n_south)

    here, end = call(
        lambda *refs: sums_kernel(scale, *refs), "sums", (tracer.shape,) * 2, (end,), [VMEM],
        cost=1 << 21, result=(1,),
    )

    before = jnp.zeros_like(total)
    for flips in ((1, 3, 2), (4, 12, 8), (28,)):
        parts = [exchange(total, lambda i, j, k=k: (i ^ k, j)) for k in flips]
        for k, part in zip(flips, parts):
            before = before + jnp.where((south ^ k) < south, part, 0.0)
        total = total + sum(parts)
    return here + before * scale, end


def solution(mesh):
    spec = P("south", "east", None)
    return jax.shard_map(
        per_device, mesh=mesh, in_specs=(spec,) * 3, out_specs=(spec,) * 2, check_vma=False
    )
```

```python
import jax
import jax.numpy as jnp
from jax import lax
from jax.experimental import pallas as pl
from jax.experimental.pallas import tpu as pltpu
from jax.sharding import PartitionSpec as P


STEPS = 4
RATE = 0.05
TILE = 8
CHUNKS = 4
W = STEPS
CORNER = (W - 1, W - 2, W - 2)

VMEM = pl.BlockSpec(memory_space=pltpu.VMEM)
ANY = pl.BlockSpec(memory_space=pl.ANY)
HBM = pl.BlockSpec(memory_space=pltpu.HBM)


def exchange(array, partner):
    n_south, n_east = lax.axis_size("south"), lax.axis_size("east")
    pairs = []
    for i in range(n_south):
        for j in range(n_east):
            p, q = partner(i, j)
            pairs.append((i * n_east + j, p * n_east + q))
    return lax.ppermute(array, ("south", "east"), pairs)


def odd(i):
    return i + 1 if i % 2 else i - 1


def south_even(i, j):
    return i ^ 1, j


def south_odd(i, j):
    p = odd(i)
    inside = 0 <= p < lax.axis_size("south")
    return (p, j) if inside else (i, j ^ 1)


def east_even(i, j):
    return i, j ^ 1


def east_odd(i, j):
    q = odd(j)
    return i, q % lax.axis_size("east")


def call(kernel, outs, operands, in_specs, scratch=(), cost=0, aliases=None, result=(), out_specs=None):
    return pl.pallas_call(
        kernel,
        out_shape=tuple(
            (jax.ShapeDtypeStruct if i in result else pltpu.VMEM)(s, jnp.float32)
            for i, s in enumerate(outs)
        ),
        in_specs=in_specs,
        out_specs=out_specs or (VMEM,) * len(outs),
        scratch_shapes=scratch,
        compiler_params=pltpu.CompilerParams(vmem_limit_bytes=16 << 20),
        cost_estimate=pl.CostEstimate(flops=cost, bytes_accessed=cost, transcendentals=0),
        input_output_aliases=aliases or {},
    )(*operands)


def low_half(shape):
    return lax.broadcasted_iota(jnp.int32, shape, len(shape) - 2) < W


def place_of():
    south, east = lax.axis_index("south"), lax.axis_index("east")
    n_south, n_east = lax.axis_size("south"), lax.axis_size("east")
    conditions = (
        south % 2 == 0, east % 2 == 0, east < n_east - 1, east > 0, south > 0, south < n_south - 1
    )
    return tuple(c.astype(jnp.int32) for c in conditions)


def start_all(copies):
    for c in copies:
        c.start()
    return copies


def wait_all(copies):
    for c in copies:
        c.wait()


def pack_kernel(tracer, flow_j, flow_i, s0, s1, e0, e1, left, right, sems):
    rows, cols = tracer.shape[0], tracer.shape[1]
    even_s, even_e = place_of()[:2]
    arrays = (tracer, flow_j, flow_i)
    copies = []

    def copy(src, dst):
        c = pltpu.make_async_copy(src, dst, sems.at[len(copies)])
        c.start()
        copies.append(c)

    for k, a in enumerate(arrays):
        copy(a.at[:, pl.ds(0, TILE)], left.at[k])
        copy(a.at[:, pl.ds(cols - TILE, TILE)], right.at[k])
    at = 0
    for a, n in zip(arrays, (W, W - 1, W - 1)):
        high = rows - n
        copy(a.at[pl.ds(even_s * high, n)], s0.at[pl.ds(at, n)])
        copy(a.at[pl.ds((1 - even_s) * high, n)], s1.at[pl.ds(at, n)])
        at += n
    for c in copies[:6]:
        c.wait()
    half = rows // 2
    low = low_half((TILE, tracer.shape[2]))

    def fold(j, carry):
        for k in range(3):
            lo = jnp.where(low, left[k, j], pltpu.roll(left[k, j + half], W, 0))
            hi = jnp.where(low, pltpu.roll(right[k, j], W, 0), right[k, j + half])
            e0[k, j] = jnp.where(even_e == 1, hi, lo)
            e1[k, j] = jnp.where(even_e == 1, lo, hi)
        return carry

    lax.fori_loop(0, half, fold, 0, unroll=4)
    for c in copies[6:]:
        c.wait()


def unfolded(e0, e1, k, j):
    _, even_e, in_right, in_left, *_ = place_of()
    low = low_half(e0.shape[2:])
    gain = jnp.where(low, in_right, in_left).astype(jnp.float32)
    a, b = e0[k, j], e1[k, j]
    right = jnp.where(even_e == 1, a, b)
    left = jnp.where(even_e == 1, b, a)
    return (
        jnp.where(low, right, pltpu.roll(left, W, 0)) * gain,
        jnp.where(low, pltpu.roll(right, W, 0), left) * gain,
    )


def corner_kernel(e0, e1, c0, c1):
    half = e0.shape[1]
    even_s = place_of()[0]
    at = 0
    for k, depth in enumerate(CORNER):
        for d in range(depth):
            first = unfolded(e0, e1, k, d)[0]
            last = unfolded(e0, e1, k, half - 1 - d)[1]
            c0[at] = jnp.where(even_s == 1, last, first)
            c1[at] = jnp.where(even_s == 1, first, last)
            at += 1


def side_mask(shape):
    in_right, in_left = place_of()[2:4]
    return jnp.where(low_half(shape), in_right, in_left).astype(jnp.float32)


def advance(below, middle, above, flow_j, flow_i, mask):
    size, cols = middle.shape[0], middle.shape[0] - TILE
    right = pltpu.roll(middle, size - 1, 0)
    left = pltpu.roll(middle, 1, 0)
    spread = below + above + left + right - 4.0 * middle
    new = middle - flow_j * (above - below) - flow_i * (right - left) + RATE * spread
    return jnp.concatenate([new[:cols], new[cols:] * mask], axis=0)


def load_kernel(tracer, flow_j, flow_i, x, fj, fi, sems):
    cols = tracer.shape[1]
    wait_all(start_all([
        pltpu.make_async_copy(src, dst.at[:, pl.ds(0, cols)], sems.at[k])
        for k, (src, dst) in enumerate(((tracer, x), (flow_j, fj), (flow_i, fi)))
    ]))


def inner_kernel(e0, e1, x_in, fj_in, fi_in, x, fj, fi, kept, end, total):
    del x_in, fj_in, fi_in
    rows, cols = end.shape[0], end.shape[1]
    half = rows // 2

    def sides(j, carry):
        for k, dst in enumerate((x, fj, fi)):
            near, far = unfolded(e0, e1, k, j)
            dst[j, cols:] = near
            dst[half + j, cols:] = far
        return carry

    lax.fori_loop(0, half, sides, 0, unroll=4)
    mask = side_mask((TILE, x.shape[2]))

    for step in range(1, STEPS + 1):
        first, last = step, rows - 1 - step
        for n in range(2):
            kept[step - 1, 0, n] = x[first - 1 + n]
            kept[step - 1, 1, n] = x[last + 1 - n]

        def body(r, carry):
            below, middle = carry[:2]
            above = x[r + 1]
            new = advance(below, middle, above, fj[r], fi[r], mask)
            if step < STEPS:
                x[r] = new
                return middle, above
            end[r] = new[:cols]
            return middle, above, carry[2] + new[:cols]

        carry = (x[first - 1], x[first])
        if step == STEPS:
            carry += (jnp.zeros((cols, x.shape[2]), jnp.float32),)
        carry = lax.fori_loop(first, last + 1, body, carry, unroll=4)
    total[...] = carry[2]


def outer_kernel(
    recv0, recv1, corner0, corner1, fj, fi, kept, inner_end, inner_total, end, total
):
    del inner_end
    rows, cols = end.shape[0], end.shape[1]
    even_s, _, _, _, has_low, has_high = place_of()
    mask = side_mask((TILE, end.shape[2]))
    so_far = inner_total[...]

    for low in (True, False):
        ours = even_s == (0 if low else 1)
        gain = (has_low if low else has_high).astype(jnp.float32)

        def halo(at, k, d):
            row = jnp.where(ours, recv0[at], recv1[at])
            if d < CORNER[k]:
                n = sum(CORNER[:k]) + d
                side = jnp.where(ours, corner0[n], corner1[n])
            else:
                side = jnp.zeros_like(mask)
            return jnp.concatenate([row, side], axis=0)

        def at_edge(d, count):
            return count - 1 - d if low else d

        field = [halo(at_edge(d, W), 0, d) * gain for d in range(W)]
        flows = [
            [halo(base + at_edge(d, W - 1), k, d) for d in range(W - 1)]
            for k, base in ((1, W), (2, 2 * W - 1))
        ]

        def flow(k, own, at):
            row = at if low else rows - 1 - at
            return flows[k][-1 - at] if at < 0 else own[row]

        values = field[::-1]
        for step in range(1, STEPS + 1):
            side = 0 if low else 1
            inward = values + [kept[step - 1, side, 0], kept[step - 1, side, 1]]
            values = []
            for n in range(1, W + 1):
                at = n - 1 + step - W
                outside, middle, inside = inward[n - 1:n + 2]
                below, above = (outside, inside) if low else (inside, outside)
                new = advance(
                    below, middle, above, flow(0, fj, at), flow(1, fi, at), mask
                )
                values.append(new * gain if at < 0 else new)
        for at, value in enumerate(values):
            end[at if low else rows - 1 - at] = value[:cols]
            so_far = so_far + value[:cols]
    total[...] = so_far


def sums_kernel(scale, end, before, here, copied, running):
    carried = before[...] * scale

    def body(j, so_far):
        row = end[j]
        copied[j] = row
        so_far = so_far + row
        scaled = so_far * scale
        here[j] = scaled
        running[j] = scaled + carried
        return so_far

    lax.fori_loop(0, end.shape[0], body, jnp.zeros(end.shape[1:], jnp.float32), unroll=4)


def finish_kernel(scale, flip, here, before, other, partial, running, buffer, sems):
    del partial
    south = lax.axis_index("south")
    chunk = here.shape[0] // CHUNKS

    @pl.when((south ^ flip) < south)
    def _():
        carried = (before[...] + other[...]) * scale
        copies = []
        for n in range(CHUNKS):
            rows = pl.ds(n * chunk, chunk)
            buffer[rows] = here[rows] + carried
            copies.append(pltpu.make_async_copy(buffer.at[rows], running.at[rows], sems.at[n]))
            copies[-1].start()
        wait_all(copies)


def per_device(tracer, flow_j, flow_i):
    rows, cols, members = tracer.shape
    south = lax.axis_index("south")
    n_south = lax.axis_size("south")
    fields = tuple(pltpu.with_memory_space_constraint(a, pltpu.HBM) for a in (tracer, flow_j, flow_i))
    edge = (3 * W - 2, cols, members)
    fold = (3, rows // 2, TILE, members)
    s0, s1, e0, e1 = call(
        pack_kernel, (edge, edge, fold, fold), fields, [HBM] * 3,
        [pltpu.VMEM((3, rows, TILE, members), jnp.float32)] * 2 + [pltpu.SemaphoreType.DMA((12,))],
    )
    e1 = exchange(e1, east_odd)
    e0 = exchange(e0, east_even)
    s1 = exchange(s1, south_odd)
    s0 = exchange(s0, south_even)

    corner = (sum(CORNER), TILE, members)
    c0, c1 = call(corner_kernel, (corner, corner), (e0, e1), [VMEM] * 2)
    c1 = exchange(c1, south_odd)
    c0 = exchange(c0, south_even)

    wide = (rows, cols + TILE, members)
    ends = (STEPS, 2, 2, cols + TILE, members)
    loaded = call(
        load_kernel, (wide,) * 3, fields, [HBM] * 3, [pltpu.SemaphoreType.DMA((3,))],
        cost=1 << 22,
    )
    _, *inner = call(
        inner_kernel, (wide,) * 3 + (ends, tracer.shape, (cols, members)),
        (e0, e1, *loaded), [VMEM] * 5, cost=1 << 22, aliases={2: 0, 3: 1, 4: 2},
    )
    end, total = call(
        outer_kernel, (tracer.shape, (cols, members)), (s0, s1, c0, c1, *inner),
        [VMEM] * 9, aliases={7: 0},
    )
    scale = 1.0 / (rows * n_south)

    before = jnp.zeros_like(total)
    for flips in ((1, 3, 2), (4, 12, 8)):
        parts = [exchange(total, lambda i, j, k=k: (i ^ k, j)) for k in flips]
        for k, part in zip(flips, parts):
            before = before + jnp.where((south ^ k) < south, part, 0.0)
        total = total + sum(parts)
    flip = 28
    other = exchange(total, lambda i, j: (i ^ flip, j))

    here, end, running_total = call(
        lambda *refs: sums_kernel(scale, *refs), (tracer.shape,) * 3, (end, before),
        [VMEM] * 2, cost=1 << 21, result=(1, 2),
    )
    (running_total,) = call(
        lambda *refs: finish_kernel(scale, flip, *refs), (tracer.shape,),
        (here, before, other, pltpu.with_memory_space_constraint(running_total, pltpu.HBM)),
        [VMEM] * 3 + [HBM],
        [pltpu.VMEM(tracer.shape, jnp.float32), pltpu.SemaphoreType.DMA((CHUNKS,))],
        aliases={3: 0}, result=(0,), out_specs=(HBM,),
    )
    return running_total, end


def solution(mesh):
    spec = P("south", "east", None)
    return jax.shard_map(
        per_device, mesh=mesh, in_specs=(spec,) * 3, out_specs=(spec,) * 2, check_vma=False
    )
```

```python
import jax
import jax.numpy as jnp
from jax import lax
from jax.experimental import pallas as pl
from jax.experimental.pallas import tpu as pltpu
from jax.sharding import PartitionSpec as P


STEPS = 4
RATE = 0.05
TILE = 8
CHUNKS = 4
W = STEPS
CORNER = (W - 1, W - 2, W - 2)

VMEM = pl.BlockSpec(memory_space=pltpu.VMEM)
ANY = pl.BlockSpec(memory_space=pl.ANY)
HBM = pl.BlockSpec(memory_space=pltpu.HBM)


def exchange(array, partner):
    n_south, n_east = lax.axis_size("south"), lax.axis_size("east")
    pairs = []
    for i in range(n_south):
        for j in range(n_east):
            p, q = partner(i, j)
            pairs.append((i * n_east + j, p * n_east + q))
    return lax.ppermute(array, ("south", "east"), pairs)


def odd(i):
    return i + 1 if i % 2 else i - 1


def south_even(i, j):
    return i ^ 1, j


def south_odd(i, j):
    p = odd(i)
    inside = 0 <= p < lax.axis_size("south")
    return (p, j) if inside else (i, j ^ 1)


def east_even(i, j):
    return i, j ^ 1


def east_odd(i, j):
    q = odd(j)
    inside = 0 <= q < lax.axis_size("east")
    return (i, q) if inside else (i ^ 1, j)


def call(kernel, outs, operands, in_specs, scratch=(), cost=0, aliases=None, result=(), out_specs=None):
    return pl.pallas_call(
        kernel,
        out_shape=tuple(
            (jax.ShapeDtypeStruct if i in result else pltpu.VMEM)(s, jnp.float32)
            for i, s in enumerate(outs)
        ),
        in_specs=in_specs,
        out_specs=out_specs or (VMEM,) * len(outs),
        scratch_shapes=scratch,
        compiler_params=pltpu.CompilerParams(vmem_limit_bytes=16 << 20),
        cost_estimate=pl.CostEstimate(flops=cost, bytes_accessed=cost, transcendentals=0),
        input_output_aliases=aliases or {},
    )(*operands)


def low_half(shape):
    return lax.broadcasted_iota(jnp.int32, shape, len(shape) - 2) < W


def place_of():
    south, east = lax.axis_index("south"), lax.axis_index("east")
    n_south, n_east = lax.axis_size("south"), lax.axis_size("east")
    conditions = (
        south % 2 == 0, east % 2 == 0, east < n_east - 1, east > 0, south > 0, south < n_south - 1
    )
    return tuple(c.astype(jnp.int32) for c in conditions)


def start_all(copies):
    for c in copies:
        c.start()
    return copies


def wait_all(copies):
    for c in copies:
        c.wait()


def pack_kernel(tracer, flow_j, flow_i, s0, s1, e0, e1, left, right, sems):
    rows, cols = tracer.shape[0], tracer.shape[1]
    even_s, even_e = place_of()[:2]
    arrays = (tracer, flow_j, flow_i)
    copies = []

    def copy(src, dst):
        c = pltpu.make_async_copy(src, dst, sems.at[len(copies)])
        c.start()
        copies.append(c)

    for k, a in enumerate(arrays):
        copy(a.at[:, pl.ds(0, TILE)], left.at[k])
        copy(a.at[:, pl.ds(cols - TILE, TILE)], right.at[k])
    at = 0
    for a, n in zip(arrays, (W, W - 1, W - 1)):
        high = rows - n
        copy(a.at[pl.ds(even_s * high, n)], s0.at[pl.ds(at, n)])
        copy(a.at[pl.ds((1 - even_s) * high, n)], s1.at[pl.ds(at, n)])
        at += n
    for c in copies[:6]:
        c.wait()
    half = rows // 2
    low = low_half((TILE, tracer.shape[2]))

    def fold(j, carry):
        for k in range(3):
            lo = jnp.where(low, left[k, j], pltpu.roll(left[k, j + half], W, 0))
            hi = jnp.where(low, pltpu.roll(right[k, j], W, 0), right[k, j + half])
            e0[k, j] = jnp.where(even_e == 1, hi, lo)
            e1[k, j] = jnp.where(even_e == 1, lo, hi)
        return carry

    lax.fori_loop(0, half, fold, 0, unroll=4)
    for c in copies[6:]:
        c.wait()


def unfolded(e0, e1, k, j):
    _, even_e, in_right, in_left, *_ = place_of()
    low = low_half(e0.shape[2:])
    gain = jnp.where(low, in_right, in_left).astype(jnp.float32)
    a, b = e0[k, j], e1[k, j]
    right = jnp.where(even_e == 1, a, b)
    left = jnp.where(even_e == 1, b, a)
    return (
        jnp.where(low, right, pltpu.roll(left, W, 0)) * gain,
        jnp.where(low, pltpu.roll(right, W, 0), left) * gain,
    )


def corner_kernel(e0, e1, c0, c1):
    half = e0.shape[1]
    even_s = place_of()[0]
    at = 0
    for k, depth in enumerate(CORNER):
        for d in range(depth):
            first = unfolded(e0, e1, k, d)[0]
            last = unfolded(e0, e1, k, half - 1 - d)[1]
            c0[at] = jnp.where(even_s == 1, last, first)
            c1[at] = jnp.where(even_s == 1, first, last)
            at += 1


def side_mask(shape):
    in_right, in_left = place_of()[2:4]
    return jnp.where(low_half(shape), in_right, in_left).astype(jnp.float32)


def advance(below, middle, above, flow_j, flow_i, mask):
    size, cols = middle.shape[0], middle.shape[0] - TILE
    right = pltpu.roll(middle, size - 1, 0)
    left = pltpu.roll(middle, 1, 0)
    spread = below + above + left + right - 4.0 * middle
    new = middle - flow_j * (above - below) - flow_i * (right - left) + RATE * spread
    return jnp.concatenate([new[:cols], new[cols:] * mask], axis=0)


def inner_kernel(tracer, flow_j, flow_i, e0, e1, fj, fi, kept, end, total, x, sems):
    rows, cols = end.shape[0], end.shape[1]
    half = rows // 2
    copies = start_all([
        pltpu.make_async_copy(src, dst.at[:, pl.ds(0, cols)], sems.at[k])
        for k, (src, dst) in enumerate(((tracer, x), (flow_j, fj), (flow_i, fi)))
    ])

    def sides(j, carry):
        for k, dst in enumerate((x, fj, fi)):
            near, far = unfolded(e0, e1, k, j)
            dst[j, cols:] = near
            dst[half + j, cols:] = far
        return carry

    lax.fori_loop(0, half, sides, 0, unroll=4)
    wait_all(copies)
    mask = side_mask((TILE, x.shape[2]))

    for step in range(1, STEPS + 1):
        first, last = step, rows - 1 - step
        for n in range(2):
            kept[step - 1, 0, n] = x[first - 1 + n]
            kept[step - 1, 1, n] = x[last + 1 - n]

        def body(r, carry):
            below, middle = carry[:2]
            above = x[r + 1]
            new = advance(below, middle, above, fj[r], fi[r], mask)
            if step < STEPS:
                x[r] = new
                return middle, above
            end[r] = new[:cols]
            return middle, above, carry[2] + new[:cols]

        carry = (x[first - 1], x[first])
        if step == STEPS:
            carry += (jnp.zeros((cols, x.shape[2]), jnp.float32),)
        carry = lax.fori_loop(first, last + 1, body, carry, unroll=4)
    total[...] = carry[2]


def outer_kernel(
    recv0, recv1, corner0, corner1, fj, fi, kept, inner_end, inner_total, end, total
):
    del inner_end
    rows, cols = end.shape[0], end.shape[1]
    even_s, _, _, _, has_low, has_high = place_of()
    mask = side_mask((TILE, end.shape[2]))
    so_far = inner_total[...]

    for low in (True, False):
        ours = even_s == (0 if low else 1)
        gain = (has_low if low else has_high).astype(jnp.float32)

        def halo(at, k, d):
            row = jnp.where(ours, recv0[at], recv1[at])
            if d < CORNER[k]:
                n = sum(CORNER[:k]) + d
                side = jnp.where(ours, corner0[n], corner1[n])
            else:
                side = jnp.zeros_like(mask)
            return jnp.concatenate([row, side], axis=0)

        def at_edge(d, count):
            return count - 1 - d if low else d

        field = [halo(at_edge(d, W), 0, d) * gain for d in range(W)]
        flows = [
            [halo(base + at_edge(d, W - 1), k, d) for d in range(W - 1)]
            for k, base in ((1, W), (2, 2 * W - 1))
        ]

        def flow(k, own, at):
            row = at if low else rows - 1 - at
            return flows[k][-1 - at] if at < 0 else own[row]

        values = field[::-1]
        for step in range(1, STEPS + 1):
            side = 0 if low else 1
            inward = values + [kept[step - 1, side, 0], kept[step - 1, side, 1]]
            values = []
            for n in range(1, W + 1):
                at = n - 1 + step - W
                outside, middle, inside = inward[n - 1:n + 2]
                below, above = (outside, inside) if low else (inside, outside)
                new = advance(
                    below, middle, above, flow(0, fj, at), flow(1, fi, at), mask
                )
                values.append(new * gain if at < 0 else new)
        for at, value in enumerate(values):
            end[at if low else rows - 1 - at] = value[:cols]
            so_far = so_far + value[:cols]
    total[...] = so_far


def sums_kernel(scale, end, before, here, copied, running):
    carried = before[...] * scale

    def body(j, so_far):
        row = end[j]
        copied[j] = row
        so_far = so_far + row
        scaled = so_far * scale
        here[j] = scaled
        running[j] = scaled + carried
        return so_far

    lax.fori_loop(0, end.shape[0], body, jnp.zeros(end.shape[1:], jnp.float32), unroll=4)


def finish_kernel(scale, flip, here, before, other, partial, running, buffer, sems):
    del partial
    south = lax.axis_index("south")
    chunk = here.shape[0] // CHUNKS

    @pl.when((south ^ flip) < south)
    def _():
        carried = (before[...] + other[...]) * scale
        copies = []
        for n in range(CHUNKS):
            rows = pl.ds(n * chunk, chunk)
            buffer[rows] = here[rows] + carried
            copies.append(pltpu.make_async_copy(buffer.at[rows], running.at[rows], sems.at[n]))
            copies[-1].start()
        wait_all(copies)


def per_device(tracer, flow_j, flow_i):
    rows, cols, members = tracer.shape
    south = lax.axis_index("south")
    n_south = lax.axis_size("south")
    fields = tuple(pltpu.with_memory_space_constraint(a, pltpu.HBM) for a in (tracer, flow_j, flow_i))
    edge = (3 * W - 2, cols, members)
    fold = (3, rows // 2, TILE, members)
    s0, s1, e0, e1 = call(
        pack_kernel, (edge, edge, fold, fold), fields, [HBM] * 3,
        [pltpu.VMEM((3, rows, TILE, members), jnp.float32)] * 2 + [pltpu.SemaphoreType.DMA((12,))],
    )
    e1 = exchange(e1, east_odd)
    e0 = exchange(e0, east_even)
    s1 = exchange(s1, south_odd)
    s0 = exchange(s0, south_even)

    corner = (sum(CORNER), TILE, members)
    c0, c1 = call(corner_kernel, (corner, corner), (e0, e1), [VMEM] * 2)
    c1 = exchange(c1, south_odd)
    c0 = exchange(c0, south_even)

    wide = (rows, cols + TILE, members)
    ends = (STEPS, 2, 2, cols + TILE, members)
    inner = call(
        inner_kernel, (wide, wide, ends, tracer.shape, (cols, members)),
        (tracer, flow_j, flow_i, e0, e1), [ANY] * 3 + [VMEM] * 2,
        [pltpu.VMEM(wide, jnp.float32), pltpu.SemaphoreType.DMA((3,))], cost=1 << 22,
    )
    end, total = call(
        outer_kernel, (tracer.shape, (cols, members)), (s0, s1, c0, c1, *inner),
        [VMEM] * 9, aliases={7: 0},
    )
    scale = 1.0 / (rows * n_south)

    before = jnp.zeros_like(total)
    for flips in ((1, 3, 2), (4, 12, 8)):
        parts = [exchange(total, lambda i, j, k=k: (i ^ k, j)) for k in flips]
        for k, part in zip(flips, parts):
            before = before + jnp.where((south ^ k) < south, part, 0.0)
        total = total + sum(parts)
    flip = 28
    other = exchange(total, lambda i, j: (i ^ flip, j))

    here, end, running_total = call(
        lambda *refs: sums_kernel(scale, *refs), (tracer.shape,) * 3, (end, before),
        [VMEM] * 2, cost=1 << 21, result=(1, 2),
    )
    (running_total,) = call(
        lambda *refs: finish_kernel(scale, flip, *refs), (tracer.shape,),
        (here, before, other, pltpu.with_memory_space_constraint(running_total, pltpu.HBM)),
        [VMEM] * 3 + [HBM],
        [pltpu.VMEM(tracer.shape, jnp.float32), pltpu.SemaphoreType.DMA((CHUNKS,))],
        aliases={3: 0}, result=(0,), out_specs=(HBM,),
    )
    return running_total, end


def solution(mesh):
    spec = P("south", "east", None)
    return jax.shard_map(
        per_device, mesh=mesh, in_specs=(spec,) * 3, out_specs=(spec,) * 2, check_vma=False
    )
```

```python
import jax
import jax.numpy as jnp
from jax import lax
from jax.experimental import pallas as pl
from jax.experimental.pallas import tpu as pltpu
from jax.sharding import PartitionSpec as P


STEPS = 4
RATE = 0.05
TILE = 8
CHUNKS = 4
W = STEPS
CORNER = (W - 1, W - 2, W - 2)

VMEM = pl.BlockSpec(memory_space=pltpu.VMEM)
ANY = pl.BlockSpec(memory_space=pl.ANY)
HBM = pl.BlockSpec(memory_space=pltpu.HBM)


def exchange(array, partner):
    n_south, n_east = lax.axis_size("south"), lax.axis_size("east")
    pairs = []
    for i in range(n_south):
        for j in range(n_east):
            p, q = partner(i, j)
            pairs.append((i * n_east + j, p * n_east + q))
    return lax.ppermute(array, ("south", "east"), pairs)


def odd(i):
    return i + 1 if i % 2 else i - 1


def south_even(i, j):
    return i ^ 1, j


def south_odd(i, j):
    p = odd(i)
    inside = 0 <= p < lax.axis_size("south")
    return (p, j) if inside else (i, j ^ 1)


def east_even(i, j):
    return i, j ^ 1


def east_odd(i, j):
    q = odd(j)
    inside = 0 <= q < lax.axis_size("east")
    return (i, q) if inside else (i ^ 1, j)


def call(kernel, outs, operands, in_specs, scratch=(), cost=0, aliases=None, result=(), out_specs=None):
    return pl.pallas_call(
        kernel,
        out_shape=tuple(
            (jax.ShapeDtypeStruct if i in result else pltpu.VMEM)(s, jnp.float32)
            for i, s in enumerate(outs)
        ),
        in_specs=in_specs,
        out_specs=out_specs or (VMEM,) * len(outs),
        scratch_shapes=scratch,
        compiler_params=pltpu.CompilerParams(vmem_limit_bytes=16 << 20),
        cost_estimate=pl.CostEstimate(flops=cost, bytes_accessed=cost, transcendentals=0),
        input_output_aliases=aliases or {},
    )(*operands)


def low_half(shape):
    return lax.broadcasted_iota(jnp.int32, shape, len(shape) - 2) < W


def place_of():
    south, east = lax.axis_index("south"), lax.axis_index("east")
    n_south, n_east = lax.axis_size("south"), lax.axis_size("east")
    conditions = (
        south % 2 == 0, east % 2 == 0, east < n_east - 1, east > 0, south > 0, south < n_south - 1
    )
    return tuple(c.astype(jnp.int32) for c in conditions)


def start_all(copies):
    for c in copies:
        c.start()
    return copies


def wait_all(copies):
    for c in copies:
        c.wait()


def pack_kernel(tracer, flow_j, flow_i, s0, s1, e0, e1, sems):
    rows, cols = tracer.shape[0], tracer.shape[1]
    even_s, even_e = place_of()[:2]
    half = rows // 2
    south = []
    at = 0
    for k, (a, n) in enumerate(zip((tracer, flow_j, flow_i), (W, W - 1, W - 1))):
        for m, (dst, edge) in enumerate(((s0, even_s), (s1, 1 - even_s))):
            src = a.at[pl.ds(edge * (rows - n), n)]
            south.append(pltpu.make_async_copy(src, dst.at[pl.ds(at, n)], sems.at[2 * k + m]))
        at += n

    def fold(right, left):
        copies = []
        for k, a in enumerate((tracer, flow_j, flow_i)):
            for m, (dst, column) in enumerate(((right, cols - W), (left, 0))):
                for h in range(2):
                    src = a.at[pl.ds(h * half, half), pl.ds(column, W)]
                    to = dst.at[k, :, pl.ds(h * W, W)]
                    copies.append(pltpu.make_async_copy(src, to, sems.at[6 + 4 * k + 2 * m + h]))
        start_all(copies)
        start_all(south)
        wait_all(copies)

    @pl.when(even_e == 1)
    def _():
        fold(e0, e1)

    @pl.when(even_e == 0)
    def _():
        fold(e1, e0)

    wait_all(south)


def unfolded(e0, e1, k, j):
    _, even_e, in_right, in_left, *_ = place_of()
    low = low_half(e0.shape[2:])
    gain = jnp.where(low, in_right, in_left).astype(jnp.float32)
    a, b = e0[k, j], e1[k, j]
    right = jnp.where(even_e == 1, a, b)
    left = jnp.where(even_e == 1, b, a)
    return (
        jnp.where(low, right, pltpu.roll(left, W, 0)) * gain,
        jnp.where(low, pltpu.roll(right, W, 0), left) * gain,
    )


def corner_kernel(e0, e1, c0, c1):
    half = e0.shape[1]
    even_s = place_of()[0]
    at = 0
    for k, depth in enumerate(CORNER):
        for d in range(depth):
            first = unfolded(e0, e1, k, d)[0]
            last = unfolded(e0, e1, k, half - 1 - d)[1]
            c0[at] = jnp.where(even_s == 1, last, first)
            c1[at] = jnp.where(even_s == 1, first, last)
            at += 1


def side_mask(shape):
    in_right, in_left = place_of()[2:4]
    return jnp.where(low_half(shape), in_right, in_left).astype(jnp.float32)


def advance(below, middle, above, flow_j, flow_i, mask):
    size, cols = middle.shape[0], middle.shape[0] - TILE
    right = pltpu.roll(middle, size - 1, 0)
    left = pltpu.roll(middle, 1, 0)
    spread = below + above + left + right - 4.0 * middle
    new = middle - flow_j * (above - below) - flow_i * (right - left) + RATE * spread
    return jnp.concatenate([new[:cols], new[cols:] * mask], axis=0)


def inner_kernel(tracer, flow_j, flow_i, e0, e1, fj, fi, kept, end, total, x, sems):
    rows, cols = end.shape[0], end.shape[1]
    half = rows // 2
    copies = start_all([
        pltpu.make_async_copy(src, dst.at[:, pl.ds(0, cols)], sems.at[k])
        for k, (src, dst) in enumerate(((tracer, x), (flow_j, fj), (flow_i, fi)))
    ])

    def sides(j, carry):
        for k, dst in enumerate((x, fj, fi)):
            near, far = unfolded(e0, e1, k, j)
            dst[j, cols:] = near
            dst[half + j, cols:] = far
        return carry

    lax.fori_loop(0, half, sides, 0, unroll=4)
    wait_all(copies)
    mask = side_mask((TILE, x.shape[2]))

    for step in range(1, STEPS + 1):
        first, last = step, rows - 1 - step
        for n in range(2):
            kept[step - 1, 0, n] = x[first - 1 + n]
            kept[step - 1, 1, n] = x[last + 1 - n]

        def body(r, carry):
            below, middle = carry[:2]
            above = x[r + 1]
            new = advance(below, middle, above, fj[r], fi[r], mask)
            if step < STEPS:
                x[r] = new
                return middle, above
            end[r] = new[:cols]
            return middle, above, carry[2] + new[:cols]

        carry = (x[first - 1], x[first])
        if step == STEPS:
            carry += (jnp.zeros((cols, x.shape[2]), jnp.float32),)
        carry = lax.fori_loop(first, last + 1, body, carry, unroll=4)
    total[...] = carry[2]


def outer_kernel(
    recv0, recv1, corner0, corner1, fj, fi, kept, inner_end, inner_total, end, total
):
    del inner_end
    rows, cols = end.shape[0], end.shape[1]
    even_s, _, _, _, has_low, has_high = place_of()
    mask = side_mask((TILE, end.shape[2]))
    so_far = inner_total[...]

    for low in (True, False):
        ours = even_s == (0 if low else 1)
        gain = (has_low if low else has_high).astype(jnp.float32)

        def halo(at, k, d):
            row = jnp.where(ours, recv0[at], recv1[at])
            if d < CORNER[k]:
                n = sum(CORNER[:k]) + d
                side = jnp.where(ours, corner0[n], corner1[n])
            else:
                side = jnp.zeros_like(mask)
            return jnp.concatenate([row, side], axis=0)

        def at_edge(d, count):
            return count - 1 - d if low else d

        field = [halo(at_edge(d, W), 0, d) * gain for d in range(W)]
        flows = [
            [halo(base + at_edge(d, W - 1), k, d) for d in range(W - 1)]
            for k, base in ((1, W), (2, 2 * W - 1))
        ]

        def flow(k, own, at):
            row = at if low else rows - 1 - at
            return flows[k][-1 - at] if at < 0 else own[row]

        values = field[::-1]
        for step in range(1, STEPS + 1):
            side = 0 if low else 1
            inward = values + [kept[step - 1, side, 0], kept[step - 1, side, 1]]
            values = []
            for n in range(1, W + 1):
                at = n - 1 + step - W
                outside, middle, inside = inward[n - 1:n + 2]
                below, above = (outside, inside) if low else (inside, outside)
                new = advance(
                    below, middle, above, flow(0, fj, at), flow(1, fi, at), mask
                )
                values.append(new * gain if at < 0 else new)
        for at, value in enumerate(values):
            end[at if low else rows - 1 - at] = value[:cols]
            so_far = so_far + value[:cols]
    total[...] = so_far


def sums_kernel(scale, end, before, here, copied, running):
    carried = before[...] * scale

    def body(j, so_far):
        row = end[j]
        copied[j] = row
        so_far = so_far + row
        scaled = so_far * scale
        here[j] = scaled
        running[j] = scaled + carried
        return so_far

    lax.fori_loop(0, end.shape[0], body, jnp.zeros(end.shape[1:], jnp.float32), unroll=4)


def finish_kernel(scale, flip, here, before, other, partial, running, buffer, sems):
    del partial
    south = lax.axis_index("south")
    chunk = here.shape[0] // CHUNKS

    @pl.when((south ^ flip) < south)
    def _():
        carried = (before[...] + other[...]) * scale
        copies = []
        for n in range(CHUNKS):
            rows = pl.ds(n * chunk, chunk)
            buffer[rows] = here[rows] + carried
            copies.append(pltpu.make_async_copy(buffer.at[rows], running.at[rows], sems.at[n]))
            copies[-1].start()
        wait_all(copies)


def per_device(tracer, flow_j, flow_i):
    rows, cols, members = tracer.shape
    south = lax.axis_index("south")
    n_south = lax.axis_size("south")
    fields = tuple(pltpu.with_memory_space_constraint(a, pltpu.HBM) for a in (tracer, flow_j, flow_i))
    edge = (3 * W - 2, cols, members)
    fold = (3, rows // 2, TILE, members)
    s0, s1, e0, e1 = call(
        pack_kernel, (edge, edge, fold, fold), fields, [HBM] * 3,
        [pltpu.SemaphoreType.DMA((18,))],
    )
    later = lax.optimization_barrier((tracer, flow_j, flow_i, e1))[:3]
    e1 = exchange(e1, east_odd)
    e0 = exchange(e0, east_even)
    s1 = exchange(s1, south_odd)
    s0 = exchange(s0, south_even)

    corner = (sum(CORNER), TILE, members)
    c0, c1 = call(corner_kernel, (corner, corner), (e0, e1), [VMEM] * 2)
    c1 = exchange(c1, south_odd)
    c0 = exchange(c0, south_even)

    wide = (rows, cols + TILE, members)
    ends = (STEPS, 2, 2, cols + TILE, members)
    inner = call(
        inner_kernel, (wide, wide, ends, tracer.shape, (cols, members)),
        (*later, e0, e1), [ANY] * 3 + [VMEM] * 2,
        [pltpu.VMEM(wide, jnp.float32), pltpu.SemaphoreType.DMA((3,))], cost=1 << 22,
    )
    end, total = call(
        outer_kernel, (tracer.shape, (cols, members)), (s0, s1, c0, c1, *inner),
        [VMEM] * 9, aliases={7: 0},
    )
    scale = 1.0 / (rows * n_south)

    before = jnp.zeros_like(total)
    for flips in ((1, 3, 2), (4, 12, 8)):
        parts = [exchange(total, lambda i, j, k=k: (i ^ k, j)) for k in flips]
        for k, part in zip(flips, parts):
            before = before + jnp.where((south ^ k) < south, part, 0.0)
        total = total + sum(parts)
    flip = 28
    other = exchange(total, lambda i, j: (i ^ flip, j))

    here, end, running_total = call(
        lambda *refs: sums_kernel(scale, *refs), (tracer.shape,) * 3, (end, before),
        [VMEM] * 2, cost=1 << 21, result=(1, 2),
    )
    (running_total,) = call(
        lambda *refs: finish_kernel(scale, flip, *refs), (tracer.shape,),
        (here, before, other, pltpu.with_memory_space_constraint(running_total, pltpu.HBM)),
        [VMEM] * 3 + [HBM],
        [pltpu.VMEM(tracer.shape, jnp.float32), pltpu.SemaphoreType.DMA((CHUNKS,))],
        aliases={3: 0}, result=(0,), out_specs=(HBM,),
    )
    return running_total, end


def solution(mesh):
    spec = P("south", "east", None)
    return jax.shard_map(
        per_device, mesh=mesh, in_specs=(spec,) * 3, out_specs=(spec,) * 2, check_vma=False
    )
```
